512 devices in a mesh: row: 16 (over x_hi, z), col: 32 (over y, x_lo, core).
Axes of the slice: x: 4 (x_hi: 2, x_lo: 2; x = x_hi * 2 + x_lo), y: 8, z: 8, core: 2. Of those that a mesh axis runs over, the one named last changes fastest.
Arguments:
- raw_records: bfloat16 [2048, 768], P(('row', 'col')), may hold values from -6 to 6
- filter_taps: float32 [129], replicated, may hold values from -0.5 to 0.5
- lag_picks: int32 [2048, 2048], P('row', 'col'), may hold values from -2 to 2
- pair_valid: int32 [2048, 2048], P('row', 'col'), may hold values 0 or 1
- clock_offset: float32 [2048], P(('row', 'col')), may hold values from -12 to 12
- clock_drift: float32 [2048], P(('row', 'col')), may hold values from -3 to 3
- var_offset: float32 [2048], P(('row', 'col')), may hold values from 0.5 to 2
- cov_cross: float32 [2048], P(('row', 'col')), may hold values from -0.4 to 0.4
- var_drift: float32 [2048], P(('row', 'col')), may hold values from 0.5 to 2
Outputs:
- pair_misfit: float32 [2048, 2048], P('row', 'col')
- new_offset: float32 [2048], P(('row', 'col'))
- new_drift: float32 [2048], P(('row', 'col'))
- new_var_offset: float32 [2048], P(('row', 'col'))
- new_cov_cross: float32 [2048], P(('row', 'col'))
- new_var_drift: float32 [2048], P(('row', 'col'))
The draws below stay inside these ranges and needn't reach their ends.
All inputs are finite; a program needn't handle non-finite values. No bound on the sum of `pair_valid` on one device may be relied on, other than what follows from the above.
Results may differ from the reference program's by a relative error of at most 0.0008.
Values may be sent and summed in bfloat16 or wider, within the bound.
No kernel may reach another device: no remote copies, remote signals or barrier semaphores. Data moves between devices by JAX's collectives and lax.ppermute only.
A program may use at most 64 MiB of HBM per device.

```python
import math
import jax
import jax.numpy as jnp
from jax import lax

SD = 4
LAG = 2
K = 129
STA = 2048
ROW_BLOCK = 128
RAW = 768
N_ROW = 16
N_COL = 32


def with_ends(drawn, rng, low, largest):
    extent = drawn.shape
    spot = [jax.random.randint(jax.random.fold_in(rng, axis), (), 0, extent[axis]) for axis in range(len(extent))]
    drawn = drawn.at[tuple(spot)].set(low)
    longest = extent.index(max(extent))
    spot[longest] = (spot[longest] + 1) % extent[longest]
    return drawn.at[tuple(spot)].set(largest)


def steps_of(key, shape, cuts, least, top_value):
    level, own = 1.0, jax.random.fold_in(key, 6)
    for dim, blocks in cuts:
        draws = jnp.exp(jax.random.uniform(jax.random.fold_in(own, dim), (blocks,), jnp.float32, least / len(cuts), top_value / len(cuts)))
        level = level * jnp.repeat(draws, shape[dim] // blocks).reshape([-1 if axis == dim else 1 for axis in range(len(shape))])
    return level


def normal_values(stream_key, dims, scale, limit, pieces=(), kind=jnp.bfloat16):
    values = scale * jax.random.normal(stream_key, dims, jnp.float32)
    if pieces:
        values = values * steps_of(stream_key, dims, pieces, -0.22, 0.18)
    return jnp.clip(values, -limit, limit).astype(kind)


def setup_inputs(seed: int = 0) -> dict:
    key_of = jax.random.split(jax.random.key(seed), 10)
    return {
        "raw_records": normal_values(key_of[0], (STA, RAW), 1.0, 6.0, ((0, 512),)),
        "filter_taps": normal_values(key_of[1], (K,), K ** -0.5, 0.5, (), jnp.float32),
        "lag_picks": with_ends(jax.random.randint(key_of[2], (STA, STA), -LAG, LAG + 1), jax.random.fold_in(key_of[2], 1), -LAG, LAG).astype(jnp.int32),
        "pair_valid": with_ends((jax.random.randint(key_of[3], (STA, STA), 0, 2) < 1).astype(jnp.int32), jax.random.fold_in(key_of[3], 1), 0, 1),
        "clock_offset": normal_values(key_of[4], (STA,), 2.0, 12.0, ((0, 512),), jnp.float32),
        "clock_drift": normal_values(key_of[5], (STA,), 0.5, 3.0, ((0, 512),), jnp.float32),
        "var_offset": jnp.clip(jnp.exp(math.log(2.0) - 1.3862944 * jax.random.uniform(key_of[6], (STA,), jnp.float32) ** steps_of(key_of[6], (STA,), ((0, 512),), -0.2, 0.2)), 0.5, 2.0),
        "cov_cross": jnp.clip(jax.random.uniform(key_of[7], (STA,), jnp.float32, -0.4, 0.4) * steps_of(key_of[7], (STA,), ((0, 512),), -0.4, 0.0), -0.4, 0.4),
        "var_drift": jnp.clip(jnp.exp(math.log(2.0) - 1.3862944 * jax.random.uniform(key_of[8], (STA,), jnp.float32) ** steps_of(key_of[8], (STA,), ((0, 512),), -0.2, 0.2)), 0.5, 2.0),
    }


EPS = 1e-06
RHO = 0.5
Q_OFFSET = 0.05
Q_DRIFT = 0.01

def whiten(raw_rows, filter_taps):
    signal = raw_rows.astype(jnp.float32)[:, None, :]
    kernel = filter_taps.astype(jnp.float32)[None, None, :]
    filtered = lax.conv_general_dilated(signal, kernel, (1,), 'VALID', dimension_numbers=('NCH', 'OIH', 'NCH'), precision=lax.Precision.HIGHEST)[:, 0, :]
    scaling = jnp.sqrt(lax.optimization_barrier(jnp.mean(filtered * filtered, axis=1, keepdims=True)) + EPS)
    return (filtered / scaling).astype(jnp.bfloat16)

def to_columns(values):
    shaped = values.reshape((N_ROW, N_COL, SD) + values.shape[1:])
    return jnp.swapaxes(shaped, 0, 1).reshape(values.shape)

def from_columns(values):
    shaped = values.reshape(N_COL, N_ROW, SD)
    return jnp.swapaxes(shaped, 0, 1).reshape(values.shape)

def fitted_lag(white_rows, column_white, pick_rows):
    window = white_rows.shape[1] - 128
    centre_rows = white_rows[:, 64:64 + window].astype(jnp.float32)
    before_lag = jnp.zeros(pick_rows.shape, jnp.float32)
    at_lag = jnp.zeros(pick_rows.shape, jnp.float32)
    after_lag = jnp.zeros(pick_rows.shape, jnp.float32)
    for shift in range(-LAG - 1, LAG + 2):
        shifted = column_white[:, 64 + shift:64 + shift + window].astype(jnp.float32)
        correl = jnp.dot(centre_rows, shifted.T, precision=lax.Precision.HIGHEST) / math.sqrt(window)
        before_lag = before_lag + jnp.where(pick_rows - 1 == shift, correl, 0.0)
        at_lag = at_lag + jnp.where(pick_rows == shift, correl, 0.0)
        after_lag = after_lag + jnp.where(pick_rows + 1 == shift, correl, 0.0)
    spread = jnp.maximum(jnp.sqrt(before_lag * before_lag + at_lag * at_lag + after_lag * after_lag), 1.0)
    return pick_rows.astype(jnp.float32) + (after_lag - before_lag) / spread

def reference(raw_records, filter_taps, lag_picks, pair_valid, clock_offset, clock_drift, var_offset, cov_cross, var_drift):
    whitened = whiten(raw_records, filter_taps)
    column_white = to_columns(whitened)
    offset_pred = clock_offset + clock_drift
    voff = var_offset + 2.0 * cov_cross + var_drift + Q_OFFSET
    vcross = cov_cross + var_drift
    vdrift = var_drift + Q_DRIFT
    column_offsets = to_columns(offset_pred)
    valid_float = pair_valid.astype(jnp.float32)

    def one_block(block_index):
        begin_at = (block_index * ROW_BLOCK).astype(jnp.int32)
        white_rows = lax.dynamic_slice_in_dim(whitened, begin_at, ROW_BLOCK, 0)
        pick_rows = lax.dynamic_slice_in_dim(lag_picks, begin_at, ROW_BLOCK, 0)
        valid_rows = lax.dynamic_slice_in_dim(valid_float, begin_at, ROW_BLOCK, 0)
        offset_rows = lax.dynamic_slice_in_dim(offset_pred, begin_at, ROW_BLOCK, 0)
        lagged = fitted_lag(white_rows, column_white, pick_rows)
        return valid_rows * (lagged - offset_rows[:, None] + column_offsets[None, :])
    pair_misfit = lax.map(one_block, jnp.arange(N_ROW, dtype=jnp.int32)).reshape(STA, STA)
    innovation = lax.optimization_barrier(jnp.sum(pair_misfit, axis=1)) + from_columns(-lax.optimization_barrier(jnp.sum(pair_misfit, axis=0)))
    pairs = lax.optimization_barrier(jnp.sum(valid_float, axis=1)) + from_columns(lax.optimization_barrier(jnp.sum(valid_float, axis=0)))
    denom = pairs * voff + RHO * STA
    share = innovation / denom
    new_offset = offset_pred + voff * share
    new_drift = clock_drift + vcross * share
    new_var_offset = voff - voff * voff * pairs / denom
    new_cov_cross = vcross - voff * vcross * pairs / denom
    new_var_drift = vdrift - vcross * vcross * pairs / denom
    return (pair_misfit, new_offset, new_drift, new_var_offset, new_cov_cross, new_var_drift)
```

```python
import math

import jax
import jax.numpy as jnp
from jax import lax
from jax.experimental import pallas as pl
from jax.experimental.pallas import tpu as pltpu
from jax.sharding import PartitionSpec as P

LAG = 2

EPS = 1e-06
RHO = 0.5
Q_OFFSET = 0.05
Q_DRIFT = 0.01

LANES = 128
OFF_LANE = 8

NT = (((1,), (1,)), ((), ()))


def three_terms(values):
    hi = values.astype(jnp.bfloat16)
    rest = values - hi.astype(jnp.float32)
    mid = rest.astype(jnp.bfloat16)
    low = (rest - mid.astype(jnp.float32)).astype(jnp.bfloat16)
    return hi, mid, low


def lane_index(shape):
    return lax.broadcasted_iota(jnp.int32, shape, 1)


def whiten_kernel(raw_ref, taps_ref, offset_ref, drift_ref, voff_ref, cross_ref, vdrift_ref,
                  row_ref, column_ref, state_ref, taps_pad):
    stations, samples = raw_ref.shape
    taps = taps_ref.shape[1]
    blocks = (samples - taps + 1) // LANES
    taps_pad[...] = jnp.zeros_like(taps_pad)
    taps_pad[0:1, 0:taps] = taps_ref[...]
    spread_taps = jnp.broadcast_to(taps_pad[0:1, :], (LANES, 2 * LANES))
    band = pltpu.roll(spread_taps, 0, 1, stride=1, stride_axis=0)
    bands = jnp.concatenate(three_terms(band), axis=0)
    raw = raw_ref[...].astype(jnp.float32)
    pieces = jnp.concatenate(
        [raw[:, b * LANES : (b + 2) * LANES] for b in range(blocks)], axis=0
    ).astype(jnp.bfloat16)
    terms = lax.dot_general(pieces, bands, NT, preferred_element_type=jnp.float32)
    filtered = terms[:, :LANES] + (terms[:, LANES : 2 * LANES] + terms[:, 2 * LANES :])
    parts = [filtered[b * stations : (b + 1) * stations] for b in range(blocks)]
    squares = parts[0] * parts[0]
    for part in parts[1:]:
        squares = squares + part * part
    mean = jnp.sum(squares, axis=1, keepdims=True) / (blocks * LANES)
    scaling = jnp.sqrt(mean + EPS)
    turned = [pltpu.roll(part / scaling, LANES // 2, 1) for part in parts]
    lane = lane_index((stations, LANES))
    rolled = [
        jnp.where(lane < LANES // 2, turned[b], turned[(b + 1) % blocks]) for b in range(blocks)
    ]
    offset_pred = offset_ref[...] + drift_ref[...]
    square = (stations, stations)
    diagonal = lax.broadcasted_iota(jnp.int32, square, 0) == lane_index(square)
    standing = jnp.sum(
        jnp.where(diagonal, jnp.broadcast_to(offset_pred, square), 0.0), axis=1, keepdims=True
    )
    for k, term in enumerate(three_terms(standing)):
        rolled[-1] = jnp.where(lane == OFF_LANE + k, term.astype(jnp.float32), rolled[-1])
    row = jnp.concatenate(rolled, axis=1).astype(jnp.bfloat16)
    for ref in (row_ref, column_ref):
        for peer in range(ref.shape[0]):
            ref[peer] = row
    cross = cross_ref[...]
    vdrift = vdrift_ref[...]
    state_ref[0:1, 0:stations] = offset_pred
    state_ref[1:2, 0:stations] = drift_ref[...]
    state_ref[2:3, 0:stations] = voff_ref[...] + 2.0 * cross + vdrift + Q_OFFSET
    state_ref[3:4, 0:stations] = cross + vdrift
    state_ref[4:5, 0:stations] = vdrift + Q_DRIFT


def pair_kernel(rows_ref, columns_ref, picks_ref, valid_ref,
                misfit_ref, row_sums_ref, column_sums_ref):
    count, width = columns_ref.shape
    window = width - LANES
    columns = columns_ref[...].astype(jnp.float32)
    shifts = range(-LAG - 1, LAG + 2)
    shifted = [
        (columns if shift == 0 else pltpu.roll(columns, (-shift) % width, 1))[:, :window]
        for shift in shifts
    ]
    stacked = jnp.concatenate(shifted, axis=0).astype(jnp.bfloat16)
    products = lax.dot_general(
        stacked, rows_ref[:, :window], NT, preferred_element_type=jnp.float32
    ) * (1.0 / math.sqrt(window))
    correl = {
        shift: products[k * count : (k + 1) * count] for k, shift in enumerate(shifts)
    }
    picks = picks_ref[...]
    shape = picks.shape
    before_lag = jnp.zeros(shape, jnp.float32)
    at_lag = before_lag
    after_lag = before_lag
    for pick in range(-LAG, LAG + 1):
        here = picks == pick
        before_lag = jnp.where(here, correl[pick - 1], before_lag)
        at_lag = jnp.where(here, correl[pick], at_lag)
        after_lag = jnp.where(here, correl[pick + 1], after_lag)
    spread = jnp.maximum(
        jnp.sqrt(before_lag * before_lag + at_lag * at_lag + after_lag * after_lag), 1.0
    )
    lagged = picks.astype(jnp.float32) + (after_lag - before_lag) / spread

    def holds_offset(lane):
        return (lane >= OFF_LANE) & (lane < OFF_LANE + 3)

    picker = jnp.where(holds_offset(lane_index((8, LANES))), 1.0, 0.0).astype(jnp.bfloat16)
    row_offsets = lax.dot_general(
        picker, rows_ref[:, window:], NT, preferred_element_type=jnp.float32
    )[0:1]
    tail = columns[:, window:]
    column_offsets = jnp.sum(
        jnp.where(holds_offset(lane_index(tail.shape)), tail, 0.0), axis=1, keepdims=True
    )
    valid = valid_ref[...].astype(jnp.float32)
    misfit = valid * (lagged - row_offsets + column_offsets)
    misfit_ref[...] = misfit
    rows = (jnp.sum(values, axis=0, keepdims=True) for values in (misfit, valid))
    row_sums_ref[...] = jnp.broadcast_to(
        jnp.concatenate(list(rows), axis=0)[None], row_sums_ref.shape
    )
    lane = lane_index(shape)
    station = lax.broadcasted_iota(jnp.int32, shape, 0)
    sums, counts = (jnp.sum(values, axis=1, keepdims=True) for values in (misfit, valid))
    laid = jnp.where(lane == station, sums, jnp.where(lane == station + count, counts, 0.0))
    column_sums_ref[...] = jnp.broadcast_to(
        jnp.sum(laid, axis=0, keepdims=True), column_sums_ref.shape
    )


def update_kernel(whole, row_sums_ref, column_sums_ref, state_ref,
                  offset_ref, drift_ref, voff_ref, cross_ref, vdrift_ref):
    stations = offset_ref.shape[1]
    rows = jnp.sum(row_sums_ref[...], axis=0)
    columns = jnp.sum(column_sums_ref[...], axis=0, keepdims=True)
    row_start = lax.axis_index("col") * stations
    column_start = lax.axis_index("row") * stations
    in_column = LANES // 2

    def from_lane(line, start):
        return pltpu.roll(line, lax.rem(LANES - start, LANES), 1)[:, :stations]

    innovation = from_lane(rows[0:1], row_start) - from_lane(columns, column_start)
    pairs = from_lane(rows[1:2], row_start) + from_lane(columns, column_start + in_column)
    offset_pred, drift, voff, vcross, vdrift = (
        state_ref[k : k + 1, 0:stations] for k in range(5)
    )
    denom = pairs * voff + RHO * whole
    share = innovation / denom
    offset_ref[...] = offset_pred + voff * share
    drift_ref[...] = drift + vcross * share
    voff_ref[...] = voff - voff * voff * pairs / denom
    cross_ref[...] = vcross - voff * vcross * pairs / denom
    vdrift_ref[...] = vdrift - vcross * vcross * pairs / denom


def in_vmem(count):
    return [pl.BlockSpec(memory_space=pltpu.VMEM)] * count


def pinned(*arrays):
    return [pltpu.with_memory_space_constraint(array, pltpu.VMEM) for array in arrays]


def local(
    raw_records,
    filter_taps,
    lag_picks,
    pair_valid,
    clock_offset,
    clock_drift,
    var_offset,
    cov_cross,
    var_drift,
):
    stations, samples = raw_records.shape
    rows_count = lax.axis_size("row")
    cols_count = lax.axis_size("col")
    taps = filter_taps.shape[0]
    width = samples - taps + 1
    in_row = stations * cols_count
    in_column = stations * rows_count
    line = (1, stations)
    for_rows, for_columns, state = pl.pallas_call(
        whiten_kernel,
        out_shape=(
            pltpu.VMEM((cols_count, stations, width), jnp.bfloat16),
            pltpu.VMEM((rows_count, stations, width), jnp.bfloat16),
            pltpu.VMEM((8, LANES), jnp.float32),
        ),
        in_specs=in_vmem(7),
        out_specs=tuple(in_vmem(3)),
        scratch_shapes=[pltpu.VMEM((8, 2 * LANES), jnp.float32)],
        name="whiten",
    )(
        raw_records,
        filter_taps.reshape(1, taps),
        clock_offset.reshape(line),
        clock_drift.reshape(line),
        var_offset.reshape(line),
        cov_cross.reshape(line),
        var_drift.reshape(line),
    )
    white_rows = lax.all_to_all(for_rows, "col", 0, 0, tiled=True).reshape(in_row, width)
    white_rows, for_columns = lax.optimization_barrier((white_rows, for_columns))
    white_columns = lax.all_to_all(for_columns, "row", 0, 0, tiled=True).reshape(in_column, width)
    misfit, row_sums, column_sums = pl.pallas_call(
        pair_kernel,
        out_shape=(
            jax.ShapeDtypeStruct((in_column, in_row), jnp.float32),
            pltpu.VMEM((cols_count, 2, LANES), jnp.float32),
            pltpu.VMEM((rows_count, LANES), jnp.float32),
        ),
        in_specs=in_vmem(4),
        out_specs=tuple(in_vmem(3)),
        name="pairs",
    )(*pinned(white_rows, white_columns, lag_picks.T, pair_valid.T))
    row_sums = lax.all_to_all(row_sums, "col", 0, 0, tiled=True)
    column_sums = lax.all_to_all(column_sums, "row", 0, 0, tiled=True)
    whole = stations * rows_count * cols_count
    updated = pl.pallas_call(
        lambda *refs: update_kernel(whole, *refs),
        out_shape=tuple(jax.ShapeDtypeStruct(line, jnp.float32) for _ in range(5)),
        in_specs=in_vmem(3),
        out_specs=tuple(in_vmem(5)),
        name="update",
    )(*pinned(row_sums, column_sums, state))
    return (misfit.T,) + tuple(values.reshape(stations) for values in updated)


def solution(mesh):
    in_specs = (
        P(("row", "col"), None),
        P(),
        P("row", "col"),
        P("row", "col"),
        P(("row", "col")),
        P(("row", "col")),
        P(("row", "col")),
        P(("row", "col")),
        P(("row", "col")),
    )
    out_specs = (
        P("row", "col"),
        P(("row", "col")),
        P(("row", "col")),
        P(("row", "col")),
        P(("row", "col")),
        P(("row", "col")),
    )
    return jax.shard_map(local, mesh=mesh, in_specs=in_specs, out_specs=out_specs, check_vma=False)
```

```python
import math

import jax
import jax.numpy as jnp
from jax import lax
from jax.experimental import pallas as pl
from jax.experimental.pallas import tpu as pltpu
from jax.sharding import PartitionSpec as P

LAG = 2

EPS = 1e-06
RHO = 0.5
Q_OFFSET = 0.05
Q_DRIFT = 0.01

LANES = 128
OFF_LANE = 8

NT = (((1,), (1,)), ((), ()))


def three_terms(values):
    hi = values.astype(jnp.bfloat16)
    rest = values - hi.astype(jnp.float32)
    mid = rest.astype(jnp.bfloat16)
    low = (rest - mid.astype(jnp.float32)).astype(jnp.bfloat16)
    return hi, mid, low


def lane_index(shape):
    return lax.broadcasted_iota(jnp.int32, shape, 1)


def whiten_kernel(raw_ref, taps_ref, offset_ref, drift_ref, voff_ref, cross_ref, vdrift_ref,
                  picks_ref, valid_ref,
                  row_ref, column_ref, state_ref, near_picks_ref, near_valid_ref, taps_pad):
    stations, samples = raw_ref.shape
    taps = taps_ref.shape[1]
    blocks = (samples - taps + 1) // LANES
    taps_pad[...] = jnp.zeros_like(taps_pad)
    taps_pad[0:1, 0:taps] = taps_ref[...]
    spread_taps = jnp.broadcast_to(taps_pad[0:1, :], (LANES, 2 * LANES))
    band = pltpu.roll(spread_taps, 0, 1, stride=1, stride_axis=0)
    bands = jnp.concatenate(three_terms(band), axis=0)
    raw = raw_ref[...].astype(jnp.float32)
    pieces = jnp.concatenate(
        [raw[:, b * LANES : (b + 2) * LANES] for b in range(blocks)], axis=0
    ).astype(jnp.bfloat16)
    terms = lax.dot_general(pieces, bands, NT, preferred_element_type=jnp.float32)
    filtered = terms[:, :LANES] + (terms[:, LANES : 2 * LANES] + terms[:, 2 * LANES :])
    parts = [filtered[b * stations : (b + 1) * stations] for b in range(blocks)]
    squares = parts[0] * parts[0]
    for part in parts[1:]:
        squares = squares + part * part
    mean = jnp.sum(squares, axis=1, keepdims=True) / (blocks * LANES)
    scaling = jnp.sqrt(mean + EPS)
    turned = [pltpu.roll(part / scaling, LANES // 2, 1) for part in parts]
    lane = lane_index((stations, LANES))
    rolled = [
        jnp.where(lane < LANES // 2, turned[b], turned[(b + 1) % blocks]) for b in range(blocks)
    ]
    offset_pred = offset_ref[...] + drift_ref[...]
    square = (stations, stations)
    diagonal = lax.broadcasted_iota(jnp.int32, square, 0) == lane_index(square)
    standing = jnp.sum(
        jnp.where(diagonal, jnp.broadcast_to(offset_pred, square), 0.0), axis=1, keepdims=True
    )
    for k, term in enumerate(three_terms(standing)):
        rolled[-1] = jnp.where(lane == OFF_LANE + k, term.astype(jnp.float32), rolled[-1])
    row = jnp.concatenate(rolled, axis=1).astype(jnp.bfloat16)
    for ref in (row_ref, column_ref):
        for peer in range(ref.shape[0]):
            ref[peer] = row
    cross = cross_ref[...]
    vdrift = vdrift_ref[...]
    state_ref[0:1, 0:stations] = offset_pred
    state_ref[1:2, 0:stations] = drift_ref[...]
    state_ref[2:3, 0:stations] = voff_ref[...] + 2.0 * cross + vdrift + Q_OFFSET
    state_ref[3:4, 0:stations] = cross + vdrift
    state_ref[4:5, 0:stations] = vdrift + Q_DRIFT
    near_picks_ref[...] = picks_ref[...]
    near_valid_ref[...] = valid_ref[...].astype(jnp.float32)


def pair_kernel(rows_ref, columns_ref, picks_ref, valid_ref,
                misfit_ref, row_sums_ref, column_sums_ref):
    count, width = columns_ref.shape
    window = width - LANES
    columns = columns_ref[...].astype(jnp.float32)
    shifts = range(-LAG - 1, LAG + 2)
    shifted = [
        (columns if shift == 0 else pltpu.roll(columns, (-shift) % width, 1))[:, :window]
        for shift in shifts
    ]
    stacked = jnp.concatenate(shifted, axis=0).astype(jnp.bfloat16)
    products = lax.dot_general(
        stacked, rows_ref[:, :window], NT, preferred_element_type=jnp.float32
    ) * (1.0 / math.sqrt(window))
    correl = {
        shift: products[k * count : (k + 1) * count] for k, shift in enumerate(shifts)
    }
    picks = picks_ref[...]
    shape = picks.shape
    before_lag = jnp.zeros(shape, jnp.float32)
    at_lag = before_lag
    after_lag = before_lag
    for pick in range(-LAG, LAG + 1):
        here = picks == pick
        before_lag = jnp.where(here, correl[pick - 1], before_lag)
        at_lag = jnp.where(here, correl[pick], at_lag)
        after_lag = jnp.where(here, correl[pick + 1], after_lag)
    spread = jnp.maximum(
        jnp.sqrt(before_lag * before_lag + at_lag * at_lag + after_lag * after_lag), 1.0
    )
    lagged = picks.astype(jnp.float32) + (after_lag - before_lag) / spread

    def holds_offset(lane):
        return (lane >= OFF_LANE) & (lane < OFF_LANE + 3)

    picker = jnp.where(holds_offset(lane_index((8, LANES))), 1.0, 0.0).astype(jnp.bfloat16)
    row_offsets = lax.dot_general(
        picker, rows_ref[:, window:], NT, preferred_element_type=jnp.float32
    )[0:1]
    tail = columns[:, window:]
    column_offsets = jnp.sum(
        jnp.where(holds_offset(lane_index(tail.shape)), tail, 0.0), axis=1, keepdims=True
    )
    valid = valid_ref[...]
    misfit = valid * (lagged - row_offsets + column_offsets)
    misfit_ref[...] = misfit
    rows = (jnp.sum(values, axis=0, keepdims=True) for values in (misfit, valid))
    row_sums_ref[...] = jnp.broadcast_to(
        jnp.concatenate(list(rows), axis=0)[None], row_sums_ref.shape
    )
    lane = lane_index(shape)
    station = lax.broadcasted_iota(jnp.int32, shape, 0)
    sums, counts = (jnp.sum(values, axis=1, keepdims=True) for values in (misfit, valid))
    laid = jnp.where(lane == station, sums, jnp.where(lane == station + count, counts, 0.0))
    column_sums_ref[...] = jnp.broadcast_to(
        jnp.sum(laid, axis=0, keepdims=True), column_sums_ref.shape
    )


def update_kernel(whole, row_sums_ref, column_sums_ref, state_ref, near_misfit_ref,
                  misfit_ref, offset_ref, drift_ref, voff_ref, cross_ref, vdrift_ref):
    misfit_ref[...] = near_misfit_ref[...]
    stations = offset_ref.shape[1]
    rows = jnp.sum(row_sums_ref[...], axis=0)
    columns = jnp.sum(column_sums_ref[...], axis=0, keepdims=True)
    row_start = lax.axis_index("col") * stations
    column_start = lax.axis_index("row") * stations
    in_column = LANES // 2

    def from_lane(line, start):
        return pltpu.roll(line, lax.rem(LANES - start, LANES), 1)[:, :stations]

    innovation = from_lane(rows[0:1], row_start) - from_lane(columns, column_start)
    pairs = from_lane(rows[1:2], row_start) + from_lane(columns, column_start + in_column)
    offset_pred, drift, voff, vcross, vdrift = (
        state_ref[k : k + 1, 0:stations] for k in range(5)
    )
    denom = pairs * voff + RHO * whole
    share = innovation / denom
    offset_ref[...] = offset_pred + voff * share
    drift_ref[...] = drift + vcross * share
    voff_ref[...] = voff - voff * voff * pairs / denom
    cross_ref[...] = vcross - voff * vcross * pairs / denom
    vdrift_ref[...] = vdrift - vcross * vcross * pairs / denom


def in_vmem(count):
    return [pl.BlockSpec(memory_space=pltpu.VMEM)] * count


def pinned(*arrays):
    return [pltpu.with_memory_space_constraint(array, pltpu.VMEM) for array in arrays]


def local(
    raw_records,
    filter_taps,
    lag_picks,
    pair_valid,
    clock_offset,
    clock_drift,
    var_offset,
    cov_cross,
    var_drift,
):
    stations, samples = raw_records.shape
    rows_count = lax.axis_size("row")
    cols_count = lax.axis_size("col")
    taps = filter_taps.shape[0]
    width = samples - taps + 1
    in_row = stations * cols_count
    in_column = stations * rows_count
    line = (1, stations)
    block = (in_column, in_row)
    for_rows, for_columns, state, picks, valid = pl.pallas_call(
        whiten_kernel,
        out_shape=(
            pltpu.VMEM((cols_count, stations, width), jnp.bfloat16),
            pltpu.VMEM((rows_count, stations, width), jnp.bfloat16),
            pltpu.VMEM((8, LANES), jnp.float32),
            pltpu.VMEM(block, jnp.int32),
            pltpu.VMEM(block, jnp.float32),
        ),
        in_specs=in_vmem(9),
        out_specs=tuple(in_vmem(5)),
        scratch_shapes=[pltpu.VMEM((8, 2 * LANES), jnp.float32)],
        name="whiten",
    )(
        raw_records,
        filter_taps.reshape(1, taps),
        clock_offset.reshape(line),
        clock_drift.reshape(line),
        var_offset.reshape(line),
        cov_cross.reshape(line),
        var_drift.reshape(line),
        lag_picks.T,
        pair_valid.T,
    )
    white_rows = lax.all_to_all(for_rows, "col", 0, 0, tiled=True).reshape(in_row, width)
    white_rows, for_columns = lax.optimization_barrier((white_rows, for_columns))
    white_columns = lax.all_to_all(for_columns, "row", 0, 0, tiled=True).reshape(in_column, width)
    misfit, row_sums, column_sums = pl.pallas_call(
        pair_kernel,
        out_shape=(
            pltpu.VMEM(block, jnp.float32),
            pltpu.VMEM((cols_count, 2, LANES), jnp.float32),
            pltpu.VMEM((rows_count, LANES), jnp.float32),
        ),
        in_specs=in_vmem(4),
        out_specs=tuple(in_vmem(3)),
        name="pairs",
    )(*pinned(white_rows, white_columns, picks, valid))
    row_sums = lax.all_to_all(row_sums, "col", 0, 0, tiled=True)
    column_sums = lax.all_to_all(column_sums, "row", 0, 0, tiled=True)
    whole = stations * rows_count * cols_count
    misfit, *updated = pl.pallas_call(
        lambda *refs: update_kernel(whole, *refs),
        out_shape=tuple(jax.ShapeDtypeStruct(shape, jnp.float32) for shape in (block,) + (line,) * 5),
        in_specs=in_vmem(4),
        out_specs=tuple(in_vmem(6)),
        name="update",
    )(*pinned(row_sums, column_sums, state, misfit))
    return (misfit.T,) + tuple(values.reshape(stations) for values in updated)


def solution(mesh):
    in_specs = (
        P(("row", "col"), None),
        P(),
        P("row", "col"),
        P("row", "col"),
        P(("row", "col")),
        P(("row", "col")),
        P(("row", "col")),
        P(("row", "col")),
        P(("row", "col")),
    )
    out_specs = (
        P("row", "col"),
        P(("row", "col")),
        P(("row", "col")),
        P(("row", "col")),
        P(("row", "col")),
        P(("row", "col")),
    )
    return jax.shard_map(local, mesh=mesh, in_specs=in_specs, out_specs=out_specs, check_vma=False)
```
